32 devices in a mesh: grp: 4 (over z), row: 4 (over y, core), col: 2 (over x).
Axes of the slice: x: 2, y: 2, z: 4, core: 2. Of those that a mesh axis runs over, the one named last changes fastest.
Arguments:
- tokens: bfloat16 [2048, 4608], P(('grp', 'row', 'col')), parts along dimension 0, may hold values from -6 to 6
- ln_gain: float32 [4608], replicated, may hold values from 0.1 to 1.9
- w_in: bfloat16 [4608, 12288], P('row', 'col'), may hold values from -0.09375 to 0.09375
- b_in: float32 [12288], P('col'), may hold values from -3 to 3
- w_out: bfloat16 [12288, 4608], P('col', 'row'), may hold values from -0.0546875 to 0.0546875
- b_out: float32 [4608], P('row'), may hold values from -3 to 3
Outputs:
- result: bfloat16 [2048, 4608], P(('grp', 'row', 'col')), parts along dimension 0
The draws below stay inside these ranges and needn't reach their ends.
There are 4 independent parts, one for each index of `grp`. The reference program is written for one: setup_inputs(seed, part) draws one part's arguments, and reference() takes and returns one part's arrays. A program takes and returns all parts, laid end to end along the dimension named above; an argument that names none is the same for every part. Nothing has to cross between parts.
All inputs are finite; a program needn't handle non-finite values.
Results may differ from the reference program's by a relative error of at most 0.0095.
Values may be sent and summed in bfloat16 or wider, within the bound.
A program may use at most 128 MiB of HBM per device.

```python
import jax
import jax.numpy as jnp
from jax import lax

D = 4608
FF = 12288
TOKENS = 512


def block_scale(own_key, dims, pieces, low, top_value):
    def one(position, blocks):
        heights = jax.random.uniform(jax.random.fold_in(jax.random.fold_in(own_key, 6), position), (blocks,), jnp.float32, low / len(pieces), top_value / len(pieces))
        return jnp.repeat(jnp.exp(heights), dims[position] // blocks).reshape((-1,) + (1,) * (len(dims) - position - 1))

    loudness = one(*pieces[0])
    for cut in pieces[1:]:
        loudness = loudness * one(*cut)
    return loudness


def normal_values(rng, shape, width, limit, shards=(), held_as=jnp.bfloat16):
    drawn = width * jax.random.normal(rng, shape, jnp.float32)
    if shards:
        drawn = drawn * block_scale(rng, shape, shards, -0.22, 0.18)
    return jnp.clip(drawn, -limit, limit).astype(held_as)


def setup_inputs(seed: int = 0, part: int = 0) -> dict:
    key_list = jax.random.split(jax.random.key(seed), 7)
    own_keys = jax.random.split(jax.random.fold_in(key_list[6], part), 7)
    tokens = normal_values(own_keys[0], (TOKENS, D), 1.0, 6.0, ((0, 8),))
    ln_gain = jnp.clip(1.0 + 0.18 * jax.random.normal(key_list[1], (D,), jnp.float32), 0.1, 1.9)
    w_in = normal_values(key_list[2], (D, FF), D ** -0.5, 0.09375, ((0, 4), (1, 2)))
    b_in = normal_values(key_list[3], (FF,), 0.5, 3.0, ((0, 2),), jnp.float32)
    w_out = normal_values(key_list[4], (FF, D), FF ** -0.5, 0.0546875, ((0, 2), (1, 4)))
    b_out = normal_values(key_list[5], (D,), 0.5, 3.0, ((0, 4),), jnp.float32)
    return {"tokens": tokens, "ln_gain": ln_gain, "w_in": w_in, "b_in": b_in, "w_out": w_out, "b_out": b_out}


def reference(tokens, ln_gain, w_in, b_in, w_out, b_out):
    values = tokens.astype(jnp.float32)
    row_mean = lax.optimization_barrier(jnp.mean(values, axis=1, keepdims=True))
    centered = values - row_mean
    row_var = lax.optimization_barrier(jnp.mean(centered * centered, axis=1, keepdims=True))
    normed = (centered * jax.lax.rsqrt(row_var + 1e-06) * ln_gain).astype(jnp.bfloat16)
    preact = jnp.dot(normed, w_in, preferred_element_type=jnp.float32) + b_in
    hidden = jax.nn.gelu(preact, approximate=False).astype(jnp.bfloat16)
    branch_out = (jnp.dot(hidden, w_out, preferred_element_type=jnp.float32) + b_out).astype(jnp.bfloat16)
    return (values + branch_out.astype(jnp.float32)).astype(jnp.bfloat16)
```

```python
import functools

import jax
import jax.numpy as jnp
from jax import lax
from jax.experimental import pallas as pl
from jax.experimental.pallas import tpu as pltpu
from jax.sharding import PartitionSpec as P

MESH = pl.DeviceIdType.MESH
F32, BF16 = jnp.float32, jnp.bfloat16
CHUNKS = 4


def tile_of(size, limit):
    return next(t for t in range(limit, 0, -128) if size % t == 0)


def block_kernel(
    tokens_ref, gain_ref, w_in_hbm, b_in_ref, w_out_hbm, b_out_ref, out_ref,
    w_in, w_out, normed, panel, mine, psend, precv, ssend, srecv, hidden, okeep, osend, orecv, branch, regrouped,
    w_sem, in_send, in_recv, fwd_send, fwd_recv, p_sem, s_sem, h_sem, o_sem, b_send, b_recv,
):
    r, c = lax.axis_index("row"), lax.axis_index("col")
    y, k = r // 2, r % 2
    partner, across = 2 * y + (1 - k), 2 * (1 - y) + k
    rows, width = tokens_ref.shape
    quarter = width // 4
    half = mine.shape[1]
    depth = w_in.shape[0]

    def remote(src, dst, send, recv, row, col=None):
        target = {"row": row} if col is None else {"row": row, "col": col}
        return pltpu.make_async_remote_copy(
            src_ref=src, dst_ref=dst, send_sem=send, recv_sem=recv, device_id=target, device_id_type=MESH
        )

    w_copies = []
    for which, (src, dst) in enumerate(((w_in_hbm, w_in), (w_out_hbm, w_out))):
        step = src.shape[0] // 4
        for part in range(4):
            cut = pl.ds(part * step, step)
            copy = pltpu.make_async_copy(src.at[cut], dst.at[cut], w_sem.at[which, part])
            copy.start()
            w_copies.append(copy)

    barrier = pltpu.get_barrier_semaphore()
    for target in ({"row": (r + 1) % 4}, {"row": (r + 2) % 4}, {"row": (r + 3) % 4}, {"col": 1 - c}):
        pl.semaphore_signal(barrier, inc=1, device_id=target, device_id_type=MESH)

    group = 16

    @pl.loop(0, rows // group)
    def _(i):
        at = pl.ds(pl.multiple_of(i * group, group), group)
        values = tokens_ref[at, :].astype(F32)
        centered = values - jnp.mean(values, axis=1, keepdims=True)
        var = jnp.mean(centered * centered, axis=1, keepdims=True)
        scaled = (centered * lax.rsqrt(var + 1e-06) * gain_ref[...]).astype(BF16)
        for q in range(4):
            normed[q, at, :] = scaled[:, q * quarter : (q + 1) * quarter]

    panel[k, y] = normed[r]
    pl.semaphore_wait(barrier, 4)

    def piece(d):
        to = (r + d) % 4
        return remote(normed.at[to], panel.at[k, y], in_send.at[d - 1], in_recv.at[k, y], to)

    for d in (1, 2, 3):
        piece(d).start()

    def forward(kk, yy):
        return remote(
            panel.at[kk, yy], panel.at[2 + kk, yy], fwd_send.at[kk, yy], fwd_recv.at[kk, yy], r, 1 - c
        )

    tile = tile_of(half, 512)
    tiles = half // tile

    def share(j):
        return remote(psend.at[j], precv.at[j], p_sem.at[0, j], p_sem.at[1, j], partner)

    def cross(j):
        return remote(ssend.at[j], srecv.at[j], s_sem.at[0, j], s_sem.at[1, j], across)

    def spread(j):
        return remote(hidden.at[j, k], hidden.at[j, k], h_sem.at[0, j], h_sem.at[1, j], partner)

    def lend(j):
        return remote(osend.at[j], orecv.at[j], o_sem.at[0, j], o_sem.at[1, j], r, 1 - c)

    def give(j, yy):
        return remote(branch.at[j, yy], regrouped.at[r], b_send.at[j, yy], b_recv.at[r], 2 * yy + j)

    def first(j):
        for yy in range(2):
            if j < 2:

                @pl.when(jnp.logical_or(k != j, y != yy))
                def _():
                    remote(panel.at[j, yy], panel.at[j, yy], in_send.at[0], in_recv.at[j, yy], across).wait_recv()

                forward(j, yy).start()
            else:
                forward(j - 2, yy).wait_recv()
        if j == 0:
            for copy in w_copies[:4]:
                copy.wait()

        @pl.loop(0, tiles)
        def _(t):
            here = pl.ds(pl.multiple_of(t * tile, tile), tile)
            there = pl.ds(pl.multiple_of((1 - k) * half + t * tile, tile), tile)
            x = panel[j].reshape(2 * rows, depth)
            psend[j, :, here] = jnp.dot(x, w_in[:, there], preferred_element_type=F32).astype(BF16)

        share(j).start()

        @pl.loop(0, tiles)
        def _(t):
            here = pl.ds(pl.multiple_of(t * tile, tile), tile)
            own = pl.ds(pl.multiple_of(k * half + t * tile, tile), tile)
            x = panel[j].reshape(2 * rows, depth)
            mine[:, here] = jnp.dot(x, w_in[:, own], preferred_element_type=F32)

        share(j).wait_recv()

        @pl.loop(0, tiles)
        def _(t):
            here = pl.ds(pl.multiple_of(t * tile, tile), tile)
            ssend[j, :, here] = (mine[:, here] + precv[j, :, here].astype(F32)).astype(BF16)

        cross(j).start()

    def second(j):
        cross(j).wait_recv()

        @pl.loop(0, tiles)
        def _(t):
            here = pl.ds(pl.multiple_of(t * tile, tile), tile)
            v = ssend[j, :, here].astype(F32) + srecv[j, :, here].astype(F32) + b_in_ref[pl.ds(k, 1), here]
            hidden[j, k, :, here] = (v * (1.0 + lax.erf(v * (0.5**0.5))) * 0.5).astype(BF16)

        spread(j).start()
        if j == 0:
            for copy in w_copies[4:]:
                copy.wait()
        total = okeep.at[j] if j < 2 else okeep.at[2]

        def down(which, t):
            here = pl.ds(pl.multiple_of(t * tile, tile), tile)
            deep = pl.ds(pl.multiple_of(which * half + t * tile, tile), tile)
            return jnp.dot(hidden[j, which, :, here], w_out[deep, :], preferred_element_type=F32)

        total[...] = down(k, 0)

        @pl.loop(1, tiles)
        def _(t):
            total[...] += down(k, t)

        remote(
            hidden.at[j, 1 - k], hidden.at[j, 1 - k], h_sem.at[0, j], h_sem.at[1, j], partner
        ).wait_recv()

        @pl.loop(0, tiles)
        def _(t):
            total[...] += down(1 - k, t)

        if j >= 2:
            osend[j - 2] = total[...].astype(BF16)
            lend(j - 2).start()

    def finish(j):
        lend(j).wait_recv()
        summed = okeep[j] + orecv[j].astype(F32) + b_out_ref[...]
        branch[j] = summed.astype(BF16).reshape(2, rows, quarter)
        for yy in range(2):
            own = jnp.logical_and(k == j, y == yy)

            @pl.when(own)
            def _():
                regrouped[r] = branch[j, yy]

            @pl.when(jnp.logical_not(own))
            def _():
                give(j, yy).start()

    for j in range(CHUNKS):
        first(j)
    for j in range(CHUNKS):
        second(j)
    for j in range(2):
        finish(j)

    for q in range(4):

        @pl.when(r != q)
        def _():
            remote(regrouped.at[q], regrouped.at[q], b_send.at[0, 0], b_recv.at[q], across).wait_recv()

        cut = pl.ds(q * quarter, quarter)
        out_ref[:, cut] = (tokens_ref[:, cut].astype(F32) + regrouped[q].astype(F32)).astype(BF16)

    for d in (1, 2, 3):
        piece(d).wait_send()
    for kk in range(2):
        for yy in range(2):
            forward(kk, yy).wait_send()
    for j in range(CHUNKS):
        share(j).wait_send()
        cross(j).wait_send()
        spread(j).wait_send()
    for j in range(2):
        lend(j).wait_send()
        for yy in range(2):

            @pl.when(jnp.logical_or(k != j, y != yy))
            def _():
                give(j, yy).wait_send()


def fused(tokens, ln_gain, w_in, b_in, w_out, b_out):
    rows, width = tokens.shape
    depth, units = w_in.shape
    half, chunk = units // 2, 2 * rows
    vmem, dma = pltpu.VMEM, pltpu.SemaphoreType.DMA
    in_vmem, in_hbm = pl.BlockSpec(memory_space=vmem), pl.BlockSpec(memory_space=pl.ANY)
    return pl.pallas_call(
        block_kernel,
        out_shape=jax.ShapeDtypeStruct((rows, width), BF16),
        in_specs=[in_vmem, in_vmem, in_hbm, in_vmem, in_hbm, in_vmem],
        out_specs=in_vmem,
        scratch_shapes=[
            vmem(w_in.shape, BF16),
            vmem(w_out.shape, BF16),
            vmem((4, rows, depth), BF16),
            vmem((CHUNKS, 2, rows, depth), BF16),
            vmem((chunk, half), F32),
            vmem((CHUNKS, chunk, half), BF16),
            vmem((CHUNKS, chunk, half), BF16),
            vmem((CHUNKS, chunk, half), BF16),
            vmem((CHUNKS, chunk, half), BF16),
            vmem((CHUNKS, 2, chunk, half), BF16),
            vmem((3, chunk, depth), F32),
            vmem((2, chunk, depth), BF16),
            vmem((2, chunk, depth), BF16),
            vmem((2, 2, rows, depth), BF16),
            vmem((4, rows, depth), BF16),
            dma((2, 4)),
            dma((3,)),
            dma((2, 2)),
            dma((2, 2)),
            dma((2, 2)),
            dma((2, CHUNKS)),
            dma((2, CHUNKS)),
            dma((2, CHUNKS)),
            dma((2, 2)),
            dma((2, 2)),
            dma((4,)),
        ],
        compiler_params=pltpu.CompilerParams(
            collective_id=0, has_side_effects=True, vmem_limit_bytes=67043328
        ),
        name="mlp_block",
    )(tokens, ln_gain.reshape(1, -1), w_in, b_in.reshape(2, -1), w_out, b_out.reshape(1, -1))


def local(tokens, ln_gain, w_in, b_in, w_out, b_out):
    values = tokens.astype(jnp.float32)
    row_mean = jnp.mean(values, axis=1, keepdims=True)
    centered = values - row_mean
    row_var = jnp.mean(centered * centered, axis=1, keepdims=True)
    normed = (centered * lax.rsqrt(row_var + 1e-06) * ln_gain).astype(jnp.bfloat16)
    own_cols = lax.all_to_all(normed, "row", split_axis=1, concat_axis=0, tiled=True)
    partial_pre = jnp.dot(
        lax.all_gather(own_cols, "col", axis=0, tiled=True),
        w_in,
        preferred_element_type=jnp.float32,
    )
    preact = lax.psum_scatter(partial_pre, "row", scatter_dimension=0, tiled=True) + b_in
    hidden = jax.nn.gelu(preact, approximate=False).astype(jnp.bfloat16)
    down_part = jnp.dot(
        lax.all_gather(hidden, "row", axis=0, tiled=True), w_out, preferred_element_type=jnp.float32
    )
    summed = lax.psum_scatter(
        down_part.astype(jnp.bfloat16), "col", scatter_dimension=0, tiled=True
    ).astype(jnp.float32)
    branch_out = (summed + b_out).astype(jnp.bfloat16)
    regrouped = lax.all_to_all(branch_out, "row", split_axis=0, concat_axis=1, tiled=True)
    return (values + regrouped.astype(jnp.float32)).astype(jnp.bfloat16)


def solution(mesh):
    in_specs = (
        P(("grp", "row", "col"), None),
        P(),
        P("row", "col"),
        P("col"),
        P("col", "row"),
        P("row"),
    )
    out_specs = P(("grp", "row", "col"), None)
    body = fused if (mesh.shape["row"], mesh.shape["col"]) == (4, 2) else local
    return jax.shard_map(body, mesh=mesh, in_specs=in_specs, out_specs=out_specs, check_vma=False)
```

```python
import functools

import jax
import jax.numpy as jnp
from jax import lax
from jax.experimental import pallas as pl
from jax.experimental.pallas import tpu as pltpu
from jax.sharding import PartitionSpec as P

MESH = pl.DeviceIdType.MESH
F32, BF16 = jnp.float32, jnp.bfloat16


def ranges(rows):
    q = rows // 4
    return [(0, 0, q), (0, q, 2 * q), (0, 2 * q, rows), (1, 0, 2 * q), (1, 2 * q, 3 * q), (1, 3 * q, rows)]


def tile_of(size, limit):
    return next(t for t in range(limit, 0, -128) if size % t == 0)


def block_kernel(
    tokens_ref, gain_ref, w_in_hbm, b_in_ref, w_out_hbm, b_out_ref, out_ref,
    w_in, w_out, normed, panel, mine, psend, precv, ssend, srecv, hidden, total, okeep, osend, orecv, branch, regrouped,
    w_sem, in_send, in_recv, fwd_sem, p_sem, s_sem, h_sem, o_sem, b_send, b_recv,
):
    r, c = lax.axis_index("row"), lax.axis_index("col")
    y, k = r // 2, r % 2
    partner, across = 2 * y + (1 - k), 2 * (1 - y) + k
    rows, width = tokens_ref.shape
    quarter = width // 4
    half = mine.shape[1]
    depth = w_in.shape[0]
    chunks = ranges(rows)
    own = [j for j, chunk in enumerate(chunks) if chunk[0] == 0]
    other = [j for j, chunk in enumerate(chunks) if chunk[0] == 1]

    def span(j):
        _, lo, hi = chunks[j]
        return pl.ds(lo, hi - lo)

    def flat(j):
        cc, lo, hi = chunks[j]
        return pl.ds(4 * (cc * rows + lo), 4 * (hi - lo))

    def remote(src, dst, send, recv, row, col=None):
        target = {"row": row} if col is None else {"row": row, "col": col}
        return pltpu.make_async_remote_copy(
            src_ref=src, dst_ref=dst, send_sem=send, recv_sem=recv, device_id=target, device_id_type=MESH
        )

    def load(which, part):
        src, dst = ((w_in_hbm, w_in), (w_out_hbm, w_out))[which]
        step = src.shape[0] // 4
        cut = pl.ds(part * step, step)
        return pltpu.make_async_copy(src.at[cut], dst.at[cut], w_sem.at[which, part])

    for part in range(4):
        load(0, part).start()

    barrier = pltpu.get_barrier_semaphore()
    for target in ({"row": (r + 1) % 4}, {"row": (r + 2) % 4}, {"row": (r + 3) % 4}, {"col": 1 - c}):
        pl.semaphore_signal(barrier, inc=1, device_id=target, device_id_type=MESH)

    def normalize(j):
        _, lo, hi = chunks[j]
        for start in range(lo, hi, rows // 4):
            at = pl.ds(start, rows // 4)
            values = tokens_ref[at, :].astype(F32)
            centered = values - jnp.mean(values, axis=1, keepdims=True)
            var = jnp.mean(centered * centered, axis=1, keepdims=True)
            scaled = (centered * lax.rsqrt(var + 1e-06) * gain_ref[...]).astype(BF16)
            for q in range(4):
                normed[q, at, :] = scaled[:, q * quarter : (q + 1) * quarter]
        panel[0, r, span(j), :] = normed[r, span(j), :]

    def piece(j, d):
        to = (r + d) % 4
        return remote(
            normed.at[to, span(j)], panel.at[0, r, span(j)], in_send.at[j, d - 1], in_recv.at[j, r], to
        )

    for j in own:
        normalize(j)
        if j == 0:
            pl.semaphore_wait(barrier, 4)
        for d in (1, 2, 3):
            piece(j, d).start()

    def forward(j):
        return remote(
            panel.at[0, :, span(j)], panel.at[1, :, span(j)], fwd_sem.at[0, j], fwd_sem.at[1, j], r, 1 - c
        )

    tile = tile_of(half, 512)
    tiles = half // tile

    def share(j):
        return remote(psend.at[flat(j)], precv.at[flat(j)], p_sem.at[0, j], p_sem.at[1, j], partner)

    def cross(j):
        return remote(ssend.at[flat(j)], srecv.at[flat(j)], s_sem.at[0, j], s_sem.at[1, j], across)

    def spread(j, which):
        held = hidden.at[which, flat(j)]
        return remote(held, held, h_sem.at[0, j], h_sem.at[1, j], partner)

    def lend(j):
        i = j - len(own)
        return remote(osend.at[:, span(j)], orecv.at[:, span(j)], o_sem.at[0, i], o_sem.at[1, i], r, 1 - c)

    def give(j, q):
        i = j - len(own)
        return remote(
            branch.at[q, span(j)], regrouped.at[r, span(j)], b_send.at[i, q], b_recv.at[i, r], q
        )

    forwarded = []

    def first(j):
        cc, lo, hi = chunks[j]
        count = 4 * (hi - lo)
        if cc == 0:
            for q in range(4):

                @pl.when(r != q)
                def _():
                    held = panel.at[0, q, span(j)]
                    remote(held, held, in_send.at[j, 0], in_recv.at[j, q], across).wait_recv()

            forward(j).start()
        else:
            for i in own:
                if i not in forwarded and chunks[i][1] < hi:
                    forward(i).wait_recv()
                    forwarded.append(i)
        if j == 0:
            for part in range(4):
                load(0, part).wait()
            for part in range(4):
                load(1, part).start()

        @pl.loop(0, tiles)
        def _(t):
            here = pl.ds(pl.multiple_of(t * tile, tile), tile)
            there = pl.ds(pl.multiple_of((1 - k) * half + t * tile, tile), tile)
            x = panel[cc, :, span(j), :].reshape(count, depth)
            psend[flat(j), here] = jnp.dot(x, w_in[:, there], preferred_element_type=F32).astype(BF16)

        share(j).start()

        @pl.loop(0, tiles)
        def _(t):
            here = pl.ds(pl.multiple_of(t * tile, tile), tile)
            mine_at = pl.ds(pl.multiple_of(k * half + t * tile, tile), tile)
            x = panel[cc, :, span(j), :].reshape(count, depth)
            mine[pl.ds(0, count), here] = jnp.dot(x, w_in[:, mine_at], preferred_element_type=F32)

        share(j).wait_recv()

        @pl.loop(0, tiles)
        def _(t):
            here = pl.ds(pl.multiple_of(t * tile, tile), tile)
            ssend[flat(j), here] = (mine[pl.ds(0, count), here] + precv[flat(j), here].astype(F32)).astype(BF16)

        cross(j).start()

    def second(j):
        cc, lo, hi = chunks[j]
        count = 4 * (hi - lo)
        cross(j).wait_recv()

        @pl.loop(0, tiles)
        def _(t):
            here = pl.ds(pl.multiple_of(t * tile, tile), tile)
            v = ssend[flat(j), here].astype(F32) + srecv[flat(j), here].astype(F32) + b_in_ref[pl.ds(k, 1), here]
            hidden[k, flat(j), here] = (v * (1.0 + lax.erf(v * (0.5**0.5))) * 0.5).astype(BF16)

        spread(j, k).start()
        if j == 0:
            for part in range(4):
                load(1, part).wait()
        acc = total.at[pl.ds(0, count)]

        def down(which, t):
            here = pl.ds(pl.multiple_of(t * tile, tile), tile)
            deep = pl.ds(pl.multiple_of(which * half + t * tile, tile), tile)
            return jnp.dot(hidden[which, flat(j), here], w_out[deep, :], preferred_element_type=F32)

        acc[...] = down(k, 0)

        @pl.loop(1, tiles)
        def _(t):
            acc[...] += down(k, t)

        spread(j, 1 - k).wait_recv()

        @pl.loop(0, tiles)
        def _(t):
            acc[...] += down(1 - k, t)

        if cc == 0:
            okeep[:, span(j), :] = acc[...].reshape(4, hi - lo, quarter)
        else:
            osend[:, span(j), :] = acc[...].astype(BF16).reshape(4, hi - lo, quarter)
            lend(j).start()

    def finish(j):
        lend(j).wait_recv()
        for q in range(4):
            summed = okeep[q, span(j), :] + orecv[q, span(j), :].astype(F32) + b_out_ref[...]
            branch[q, span(j), :] = summed.astype(BF16)
        for q in range(4):

            @pl.when(r == q)
            def _():
                regrouped[r, span(j), :] = branch[q, span(j), :]

            @pl.when(r != q)
            def _():
                give(j, q).start()

    def settle(j):
        i = j - len(own)
        for q in range(4):

            @pl.when(r != q)
            def _():
                held = regrouped.at[q, span(j)]
                remote(held, held, b_send.at[i, 0], b_recv.at[i, q], across).wait_recv()

            cut = pl.ds(q * quarter, quarter)
            out_ref[span(j), cut] = (
                tokens_ref[span(j), cut].astype(F32) + regrouped[q, span(j), :].astype(F32)
            ).astype(BF16)

    for j in range(len(chunks)):
        first(j)
    for j in range(len(chunks)):
        second(j)
        if j > len(own):
            finish(j - 1)
    for j in other[:-2]:
        settle(j)
    finish(other[-1])
    for j in other[-2:]:
        settle(j)

    for j in own:
        for d in (1, 2, 3):
            piece(j, d).wait_send()
        forward(j).wait_send()
    for j in range(len(chunks)):
        share(j).wait_send()
        cross(j).wait_send()
        spread(j, k).wait_send()
    for j in other:
        lend(j).wait_send()
        for q in range(4):

            @pl.when(r != q)
            def _():
                give(j, q).wait_send()


def fused(tokens, ln_gain, w_in, b_in, w_out, b_out):
    rows, width = tokens.shape
    depth, units = w_in.shape
    half = units // 2
    chunks = ranges(rows)
    steps = len(chunks)
    kept = sum(chunk[0] == 0 for chunk in chunks)
    most = 4 * max(hi - lo for _, lo, hi in chunks)
    vmem, dma = pltpu.VMEM, pltpu.SemaphoreType.DMA
    in_vmem, in_hbm = pl.BlockSpec(memory_space=vmem), pl.BlockSpec(memory_space=pl.ANY)
    return pl.pallas_call(
        block_kernel,
        out_shape=jax.ShapeDtypeStruct((rows, width), BF16),
        in_specs=[in_vmem, in_vmem, in_hbm, in_vmem, in_hbm, in_vmem],
        out_specs=in_vmem,
        scratch_shapes=[
            vmem(w_in.shape, BF16),
            vmem(w_out.shape, BF16),
            vmem((4, rows, depth), BF16),
            vmem((2, 4, rows, depth), BF16),
            vmem((most, half), F32),
            vmem((8 * rows, half), BF16),
            vmem((8 * rows, half), BF16),
            vmem((8 * rows, half), BF16),
            vmem((8 * rows, half), BF16),
            vmem((2, 8 * rows, half), BF16),
            vmem((most, depth), F32),
            vmem((4, rows, depth), F32),
            vmem((4, rows, depth), BF16),
            vmem((4, rows, depth), BF16),
            vmem((4, rows, depth), BF16),
            vmem((4, rows, depth), BF16),
            dma((2, 4)),
            dma((kept, 3)),
            dma((kept, 4)),
            dma((2, kept)),
            dma((2, steps)),
            dma((2, steps)),
            dma((2, steps)),
            dma((2, steps - kept)),
            dma((steps - kept, 4)),
            dma((steps - kept, 4)),
        ],
        compiler_params=pltpu.CompilerParams(
            collective_id=0, has_side_effects=True, vmem_limit_bytes=67043328
        ),
        name="mlp_block",
    )(tokens, ln_gain.reshape(1, -1), w_in, b_in.reshape(2, -1), w_out, b_out.reshape(1, -1))


def local(tokens, ln_gain, w_in, b_in, w_out, b_out):
    values = tokens.astype(jnp.float32)
    row_mean = jnp.mean(values, axis=1, keepdims=True)
    centered = values - row_mean
    row_var = jnp.mean(centered * centered, axis=1, keepdims=True)
    normed = (centered * lax.rsqrt(row_var + 1e-06) * ln_gain).astype(jnp.bfloat16)
    own_cols = lax.all_to_all(normed, "row", split_axis=1, concat_axis=0, tiled=True)
    partial_pre = jnp.dot(
        lax.all_gather(own_cols, "col", axis=0, tiled=True),
        w_in,
        preferred_element_type=jnp.float32,
    )
    preact = lax.psum_scatter(partial_pre, "row", scatter_dimension=0, tiled=True) + b_in
    hidden = jax.nn.gelu(preact, approximate=False).astype(jnp.bfloat16)
    down_part = jnp.dot(
        lax.all_gather(hidden, "row", axis=0, tiled=True), w_out, preferred_element_type=jnp.float32
    )
    summed = lax.psum_scatter(
        down_part.astype(jnp.bfloat16), "col", scatter_dimension=0, tiled=True
    ).astype(jnp.float32)
    branch_out = (summed + b_out).astype(jnp.bfloat16)
    regrouped = lax.all_to_all(branch_out, "row", split_axis=0, concat_axis=1, tiled=True)
    return (values + regrouped.astype(jnp.float32)).astype(jnp.bfloat16)


def solution(mesh):
    in_specs = (
        P(("grp", "row", "col"), None),
        P(),
        P("row", "col"),
        P("col"),
        P("col", "row"),
        P("row"),
    )
    out_specs = P(("grp", "row", "col"), None)
    body = fused if (mesh.shape["row"], mesh.shape["col"]) == (4, 2) else local
    return jax.shard_map(body, mesh=mesh, in_specs=in_specs, out_specs=out_specs, check_vma=False)
```
